256 devices in a mesh: row: 8 (over y, x_hi), theta: 4 (over x_lo, core), gz: 8 (over z).
Axes of the slice: x: 4 (x_hi: 2, x_lo: 2; x = x_hi * 2 + x_lo), y: 4, z: 8, core: 2. Of those that a mesh axis runs over, the one named last changes fastest.
Arguments:
- state_start: float32 [6, 32, 256, 1024], P(None, 'row', 'gz', 'theta'), may hold values from -1.2 to 1.2
- state_section: float32 [6, 32, 256, 1024], P(None, 'row', 'gz', 'theta'), may hold values from -1.5 to 4, as said below
- phase: int32 [32, 256, 1024], P('row', 'gz', 'theta'), may hold values 0 or 1
- cutoff: int32 [4], replicated, may hold values from 1 to 63
Outputs:
- state_next: float32 [6, 32, 256, 1024], P(None, 'row', 'gz', 'theta')
The draws below stay inside these ranges and needn't reach their ends.
Inputs may be any that keep to these rules, and one draw needn't show every extreme that they name: `state_section`: channel 0 (density) lies in 0.5 to 2.0, channels 1 to 3 (momenta) in -1.5 to 1.5, channel 4 (total energy) in 2.5 to 4.0, channel 5 (jet mass density) in 0 to 1.0.
All inputs are finite; a program needn't handle non-finite values. No bound on the sum of `phase` on one device may be relied on, other than what follows from the above.
Results may differ from the reference program's by a relative error of at most 0.0003.
Values sent between devices are 32-bit elements; how exact they have to be, the bound alone decides.
No kernel may reach another device: no remote copies, remote signals or barrier semaphores. Data moves between devices by JAX's collectives and lax.ppermute only.
A program may use at most 64 MiB of HBM per device.

```python
import math
import jax
import jax.numpy as jnp
from jax import lax

NT = 1024
NF = 4
KMODES = 64
NR = 32
NZ = 256


def draw_state_section(key, part):
    subkeys = jax.random.split(jax.random.fold_in(key, 11), 4)
    grid_shape = (NR, NZ, NT)
    density = jax.random.uniform(subkeys[0], grid_shape, minval=0.5, maxval=2.0)
    momenta = jnp.clip(0.3 * jax.random.normal(subkeys[1], (3, NR, NZ, NT)), -1.5, 1.5)
    energy = jax.random.uniform(subkeys[2], grid_shape, minval=2.5, maxval=4.0)
    jet_mass = jax.random.uniform(subkeys[3], grid_shape, minval=0.0, maxval=1.0)
    return jnp.concatenate([density[None], momenta, energy[None], jet_mass[None]], 0).astype(jnp.float32)


def place_ends(values, key, least, largest):
    longest = values.shape.index(max(values.shape))
    spots = []
    for shift in (0, 1):
        where = [jax.random.randint(jax.random.fold_in(key, axis), (), 0, length) for axis, length in enumerate(values.shape)]
        where[longest] = (where[longest] + shift) % values.shape[longest]
        spots.append(tuple(where))
    return values.at[spots[0]].set(least).at[spots[1]].set(largest)


def block_scale(own_key, dims, cuts, low, high):
    def one(position, parts):
        draws = jax.random.uniform(jax.random.fold_in(jax.random.fold_in(own_key, 6), position), (parts,), jnp.float32, low / len(cuts), high / len(cuts))
        return jnp.repeat(jnp.exp(draws), dims[position] // parts).reshape((-1,) + (1,) * (len(dims) - position - 1))

    gain = one(*cuts[0])
    for cut in cuts[1:]:
        gain = gain * one(*cut)
    return gain


def gaussian(rng, dims, scale, most, pieces=(), kind=jnp.bfloat16):
    gain = block_scale(rng, dims, pieces, -0.22, 0.18) if pieces else 1.0
    result = jax.random.normal(rng, dims, jnp.float32) * scale * gain
    return jnp.minimum(jnp.maximum(result, -most), most).astype(kind)


def setup_inputs(seed: int = 0) -> dict:
    splits = jax.random.split(jax.random.key(seed), 5)
    return {
        "state_start": gaussian(splits[0], (6, NR, NZ, NT), 0.2, 1.2, ((1, 8), (2, 8), (3, 4)), jnp.float32),
        "state_section": draw_state_section(jax.random.fold_in(splits[4], 71), 0),
        "phase": place_ends((jax.random.randint(splits[2], (NR, NZ, NT), 0, 3) < 1).astype(jnp.int32), jax.random.fold_in(splits[2], 1), 0, 1),
        "cutoff": place_ends(jax.random.randint(splits[3], (NF,), 1, KMODES), jax.random.fold_in(splits[3], 1), 1, KMODES - 1).astype(jnp.int32),
    }


split_speed = 10.0
time_step = 0.05
weno_epsilon = 1e-6
liquid_ratio = 4.4
gas_ratio = 1.4
liquid_stiffness = 0.6


def pressure_of(state, phase):
    density = state[0]
    kinetic = 0.5 * (state[1] * state[1] + state[2] * state[2] + state[3] * state[3]) / density
    liquid = phase == 1
    heat_ratio = jnp.where(liquid, liquid_ratio, gas_ratio)
    stiffness = jnp.where(liquid, liquid_stiffness, 0.0)
    return (heat_ratio - 1.0) * (state[4] - kinetic) - heat_ratio * stiffness


def weno_face(far_left, near_left, centre, near_right, far_right):
    smooth_left = 13.0 / 12.0 * (far_left - 2.0 * near_left + centre) ** 2 + 0.25 * (far_left - 4.0 * near_left + 3.0 * centre) ** 2
    smooth_mid = 13.0 / 12.0 * (near_left - 2.0 * centre + near_right) ** 2 + 0.25 * (near_left - near_right) ** 2
    smooth_right = 13.0 / 12.0 * (centre - 2.0 * near_right + far_right) ** 2 + 0.25 * (3.0 * centre - 4.0 * near_right + far_right) ** 2
    weight_left = 0.1 / (weno_epsilon + smooth_left) ** 2
    weight_mid = 0.6 / (weno_epsilon + smooth_mid) ** 2
    weight_right = 0.3 / (weno_epsilon + smooth_right) ** 2
    weight_sum = weight_left + weight_mid + weight_right
    value_left = (2.0 * far_left - 7.0 * near_left + 11.0 * centre) / 6.0
    value_mid = (-near_left + 5.0 * centre + 2.0 * near_right) / 6.0
    value_right = (2.0 * centre + 5.0 * near_right - far_right) / 6.0
    return (weight_left * value_left + weight_mid * value_mid + weight_right * value_right) / weight_sum


def face_fluxes(padded_line, array_axis, component):
    density = padded_line[0]
    velocity = padded_line[component] / density
    pressure_field = padded_line[6]
    conserved = padded_line[:6]
    flux_rows = [conserved[channel] * velocity for channel in range(6)]
    flux_rows[component] = flux_rows[component] + pressure_field
    flux_rows[4] = flux_rows[4] + pressure_field * velocity
    physical = jnp.stack(flux_rows)
    upward = 0.5 * (physical + split_speed * conserved)
    downward = 0.5 * (physical - split_speed * conserved)
    face_count = padded_line.shape[array_axis] - 5

    def shifted(values, offset):
        return lax.slice_in_dim(values, offset, offset + face_count, axis=array_axis)

    upwind_part = weno_face(shifted(upward, 0), shifted(upward, 1), shifted(upward, 2), shifted(upward, 3), shifted(upward, 4))
    downwind_part = weno_face(shifted(downward, 5), shifted(downward, 4), shifted(downward, 3), shifted(downward, 2), shifted(downward, 1))
    return upwind_part + downwind_part


def tendency(centre_cells, radial_line, axial_line, azimuth_line, cycle_start):
    cycle_count = centre_cells.shape[1]
    radial_flux = face_fluxes(radial_line, 1, 1)
    axial_flux = face_fluxes(axial_line, 2, 3)
    azimuth_flux = face_fluxes(azimuth_line, 3, 2)
    cycle_index = (cycle_start + lax.iota(jnp.int32, cycle_count + 1)).astype(centre_cells.dtype)
    face_radius = cycle_index[None, :, None, None]
    cell_radius = face_radius[:, :-1] + 0.5
    weighted = face_radius * radial_flux
    div_radial = (weighted[:, 1:] - weighted[:, :-1]) / cell_radius
    div_axial = axial_flux[:, :, 1:] - axial_flux[:, :, :-1]
    angle_step = 2.0 * math.pi / NT
    div_azimuth = (azimuth_flux[..., 1:] - azimuth_flux[..., :-1]) / (cell_radius * angle_step)
    density = centre_cells[0]
    swirl_speed = centre_cells[2] / density
    radius = cell_radius[0]
    source_radial = (centre_cells[2] * swirl_speed + centre_cells[6]) / radius
    source_swirl = -centre_cells[1] * swirl_speed / radius
    zero_field = jnp.zeros_like(density)
    source = jnp.stack([zero_field, source_radial, source_swirl, zero_field, zero_field, zero_field])
    return source - div_radial - div_axial - div_azimuth


def across_axis(partner):
    sign_flip = jnp.array([1.0, -1.0, -1.0, 1.0, 1.0, 1.0, 1.0], partner.dtype)[:, None, None, None]
    return partner[:, ::-1] * sign_flip


def reference(state_start, state_section, phase, cutoff):
    pressure_field = pressure_of(state_section, phase)
    fields = jnp.concatenate([state_section, pressure_field[None]], 0)
    total_depth = fields.shape[2]
    block_size = math.gcd(total_depth, 8)
    block_count = total_depth // block_size

    def one_block(number):
        positions = (number * block_size - 3 + lax.iota(jnp.int32, block_size + 6)) % total_depth
        axial_line = jnp.take(fields, positions.astype(jnp.int32), axis=2)
        centre_cells = axial_line[:, :, 3:-3]
        partner = jnp.roll(centre_cells[:, 0:3], -(NT // 2), axis=3)
        outer_rim = jnp.repeat(centre_cells[:, -1:], 3, axis=1)
        radial_line = jnp.concatenate([across_axis(partner), centre_cells, outer_rim], 1)
        azimuth_line = jnp.concatenate([centre_cells[..., -3:], centre_cells, centre_cells[..., :3]], 3)
        tendencies = tendency(centre_cells, radial_line, axial_line, azimuth_line, 0)
        start_index = (number * block_size).astype(jnp.int32)
        start_block = lax.dynamic_slice_in_dim(state_start, start_index, block_size, 2)
        section_block = lax.dynamic_slice_in_dim(state_section, start_index, block_size, 2)
        return 0.75 * start_block + 0.25 * (section_block + time_step * tendencies)

    block_results = lax.map(one_block, lax.iota(jnp.int32, block_count))
    advanced = jnp.moveaxis(block_results, 0, 2).reshape(state_start.shape)
    inner_block = advanced[:, :NF]
    spectrum = jnp.fft.rfft(inner_block, axis=3)
    mode_index = lax.iota(jnp.int32, NT // 2 + 1)
    kept_modes = mode_index[None, :] <= cutoff[:, None]
    filtered = jnp.fft.irfft(spectrum * kept_modes[None, :, None, :], n=NT, axis=3).astype(advanced.dtype)
    return jnp.concatenate([filtered, advanced[:, NF:]], 1)
```

```python
import math

import jax
import jax.numpy as jnp
from jax import lax
from jax.experimental import pallas as pl
from jax.experimental.pallas import tpu as pltpu
from jax.sharding import PartitionSpec as P


NT = 1024
KMODES = 64
LANES = 128
SUB = 8

split_speed = 10.0
time_step = 0.05
weno_epsilon = 1e-06
liquid_ratio = 4.4
gas_ratio = 1.4
liquid_stiffness = 0.6
f32 = jnp.float32


def pressure_at(q, phase):
    kinetic = 0.5 * (q[1] * q[1] + q[2] * q[2] + q[3] * q[3]) / q[0]
    liquid = phase == 1
    heat_ratio = jnp.where(liquid, liquid_ratio, gas_ratio)
    stiffness = jnp.where(liquid, liquid_stiffness, 0.0)
    return (heat_ratio - 1.0) * (q[4] - kinetic) - heat_ratio * stiffness


def doubled_fluxes(q, channel, component, velocity):
    physical = q[channel] * velocity
    if channel == component:
        physical = physical + q[6]
    if channel == 4:
        physical = (q[4] + q[6]) * velocity
    carried = split_speed * q[channel]
    return physical + carried, physical - carried


def curvature(before, centre, after):
    step_low = centre - before
    step_high = after - centre
    second = step_high - step_low
    half = 0.5 * second
    base = (13.0 / 12.0) * (second * second) + 4.0 * weno_epsilon
    left = step_high + half
    mid = step_low + half
    right = step_low - half
    return left * left + base, mid * mid + base, right * right + base, second


def weighted_shift(beta_0, beta_1, beta_2, third_0, third_2):
    p = beta_1 * beta_2
    r = beta_0 * beta_2
    s = beta_0 * beta_1
    c_0 = p * p
    c_1 = 6.0 * (r * r)
    c_2 = 3.0 * (s * s)
    return ((c_0 + c_0) * third_0 + c_2 * third_2) / (c_0 + c_1 + c_2)


def centred(near, centre, far):
    return 5.0 * centre - near + 2.0 * far


SEG = 32
EXT = SEG + 2 * SUB
ROWS = EXT + SUB


def sweep(load, component, emit, scratch):
    up_ref, down_ref, face_ref = scratch[0], scratch[1], scratch[2]
    lists = scratch[3:]
    blocks = EXT // SUB
    cells = [[load(c, b) for c in range(7)] for b in range(blocks)]
    speed = [q[component] / q[0] for q in cells]
    for c in range(6):
        for b in range(blocks):
            up, down = doubled_fluxes(cells[b], c, component, speed[b])
            up_ref[c, b * SUB : (b + 1) * SUB, :] = up
            down_ref[c, b * SUB : (b + 1) * SUB, :] = down
    for c in range(6):
        for side, ref in ((0, up_ref), (1, down_ref)):
            for b in range(5):
                row = 6 + b * SUB
                vals = curvature(
                    ref[c, row - 1 : row - 1 + SUB, :],
                    ref[c, row : row + SUB, :],
                    ref[c, row + 1 : row + 1 + SUB, :],
                )
                for k in range(4):
                    lists[side * 4 + k][c, row : row + SUB, :] = vals[k]
    for c in range(6):
        for b in range(5):
            j = SUB + b * SUB

            def at(ref, off):
                return ref[c, j + off : j + off + SUB, :]

            la, ca, ra, sa = lists[0:4]
            s0, s1, s2 = at(sa, -2), at(sa, -1), at(sa, 0)
            up_part = weighted_shift(at(la, -2), at(ca, -1), at(ra, 0), s0 - s1, s1 - s2)
            lb, cb, rb, sb = lists[4:8]
            s0, s1, s2 = at(sb, 1), at(sb, 0), at(sb, -1)
            down_part = weighted_shift(at(rb, 1), at(cb, 0), at(lb, -1), s0 - s1, s1 - s2)
            total = up_part + down_part
            total = total + centred(at(up_ref, -2), at(up_ref, -1), at(up_ref, 0))
            total = total + centred(at(down_ref, 1), at(down_ref, 0), at(down_ref, -1))
            face_ref[c, b * SUB : (b + 1) * SUB, :] = total
        for b in range(SEG // SUB):
            low = face_ref[c, b * SUB : (b + 1) * SUB, :]
            high = face_ref[c, b * SUB + 1 : b * SUB + 1 + SUB, :]
            emit(c, b, high - low)


def sweep_scratch():
    return [pltpu.VMEM((6, ROWS, LANES), f32) for _ in range(11)]


def pack_body(section_ref, phase_ref, bottom_ref, top_ref, pressure_ref, first_ref, last_ref):
    cycles, depth = section_ref.shape[1], section_ref.shape[2]
    for k in range(cycles):
        q = [section_ref[c, k] for c in range(6)]
        q.append(pressure_at(q, phase_ref[k]))
        pressure_ref[k] = q[6]
        for c in range(7):
            if k < 3:
                bottom_ref[c, k] = q[c]
            if k > 0:
                top_ref[c, k - 1] = q[c]
            first_ref[c * cycles + k] = q[c][:SUB]
            last_ref[c * cycles + k] = q[c][depth - SUB :]


def pack_call(section, phase):
    _, cycles, depth, width = section.shape
    layers = jax.ShapeDtypeStruct((7, 3, depth, width), f32)
    edge = jax.ShapeDtypeStruct((7 * cycles, SUB, width), f32)
    pressure = jax.ShapeDtypeStruct((cycles, depth, width), f32)
    return pl.pallas_call(pack_body, out_shape=(layers, layers, pressure, edge, edge), name="pack")(
        section, phase
    )


def turn_body(section_ref, pressure_ref, turned_ref, first_ref, last_ref):
    cycles, depth, width = pressure_ref.shape
    for c in range(7):
        q = section_ref[c] if c < 6 else pressure_ref[...]
        q = q.reshape(cycles * depth, width)
        for h in range(width // LANES):
            t = q[:, h * LANES : (h + 1) * LANES].T
            turned_ref[c, h * LANES : (h + 1) * LANES, :] = t
            if h == 0:
                first_ref[c] = t[:SUB]
            if h == width // LANES - 1:
                last_ref[c] = t[LANES - SUB :]


def turn_call(section, pressure):
    cycles, depth, width = pressure.shape
    turned = jax.ShapeDtypeStruct((7, width, cycles * depth), f32)
    edge = jax.ShapeDtypeStruct((7, SUB, cycles * depth), f32)
    return pl.pallas_call(turn_body, out_shape=(turned, edge, edge), name="turn")(section, pressure)


def axial_body(start_ref, section_ref, pressure_ref, before_ref, after_ref, out_ref, *scratch):
    cycles, _, width = pressure_ref.shape
    first = lax.axis_index("row") * cycles

    @pl.loop(0, cycles)
    def _(k):
        radius = (first + k).astype(f32) + 0.5
        for h in range(width // LANES):
            lanes = slice(h * LANES, (h + 1) * LANES)

            def load(c, b):
                if b == 0:
                    return before_ref[c * cycles + k, :, lanes]
                if b == EXT // SUB - 1:
                    return after_ref[c * cycles + k, :, lanes]
                rows = slice((b - 1) * SUB, b * SUB)
                return section_ref[c, k, rows, lanes] if c < 6 else pressure_ref[k, rows, lanes]

            def emit(c, b, change):
                rows = slice(b * SUB, (b + 1) * SUB)
                value = 0.25 * section_ref[c, k, rows, lanes] - (0.25 * time_step / 12.0) * change
                if c in (1, 2):
                    swirl = section_ref[2, k, rows, lanes] / section_ref[0, k, rows, lanes]
                    if c == 1:
                        source = section_ref[2, k, rows, lanes] * swirl + pressure_ref[k, rows, lanes]
                    else:
                        source = -section_ref[1, k, rows, lanes] * swirl
                    value = value + (0.25 * time_step) * (source / radius)
                out_ref[c, k, rows, lanes] = 0.75 * start_ref[c, k, rows, lanes] + value

            sweep(load, 3, emit, scratch)


def axial_call(start, section, pressure, before, after):
    return pl.pallas_call(
        axial_body,
        out_shape=jax.ShapeDtypeStruct(section.shape, f32),
        scratch_shapes=sweep_scratch(),
        name="axial",
    )(start, section, pressure, before, after)


def swirl_body(partial_ref, turned_ref, before_ref, after_ref, out_ref, ext_ref, div_ref, *scratch):
    width = turned_ref.shape[1]
    cycles, depth = partial_ref.shape[1], partial_ref.shape[2]
    first = lax.axis_index("row") * cycles
    for c in range(7):
        ext_ref[c, 0:SUB, :] = before_ref[c]
        ext_ref[c, SUB + width : 2 * SUB + width, :] = after_ref[c]
        ext_ref[c, SUB : SUB + width, :] = turned_ref[c]

    @pl.loop(0, width // SEG)
    def _(n):
        origin = pl.multiple_of(n * SEG, SEG)

        def load(c, b):
            return ext_ref[c, pl.ds(origin + b * SUB, SUB), :]

        def emit(c, b, change):
            div_ref[c, pl.ds(origin + b * SUB, SUB), :] = change

        sweep(load, 2, emit, scratch)

    angle_step = 2.0 * math.pi / NT
    for c in range(6):
        for h in range(width // LANES):
            lanes = slice(h * LANES, (h + 1) * LANES)
            div = div_ref[c, h * LANES : (h + 1) * LANES, :].T
            div = div.reshape(cycles, depth, LANES)
            for k in range(cycles):
                radius = (first + k).astype(f32) + 0.5
                scale = (0.25 * time_step / 12.0) / (radius * angle_step)
                out_ref[c, k, :, lanes] = partial_ref[c, k, :, lanes] - scale * div[k]


def swirl_call(partial, turned, before, after):
    width = turned.shape[1]
    return pl.pallas_call(
        swirl_body,
        out_shape=jax.ShapeDtypeStruct(partial.shape, f32),
        scratch_shapes=[
            pltpu.VMEM((7, width + 2 * SUB, LANES), f32),
            pltpu.VMEM((6, width, LANES), f32),
        ]
        + sweep_scratch(),
        name="swirl",
    )(partial, turned, before, after)


def radial_parts(load, cell_list):
    cells = {k: [load(c, k) for c in range(7)] for k in cell_list}
    speed = {k: q[1] / q[0] for k, q in cells.items()}
    for c in range(6):
        pairs = {k: doubled_fluxes(cells[k], c, 1, speed[k]) for k in cell_list}
        yield c, {k: v[0] for k, v in pairs.items()}, {k: v[1] for k, v in pairs.items()}


def face_up(y, j, curves):
    s0, s1, s2 = curves[j - 2][3], curves[j - 1][3], curves[j][3]
    shift = weighted_shift(curves[j - 2][0], curves[j - 1][1], curves[j][2], s0 - s1, s1 - s2)
    return shift + centred(y[j - 2], y[j - 1], y[j])


def face_down(y, j, curves):
    s0, s1, s2 = curves[j + 1][3], curves[j][3], curves[j - 1][3]
    shift = weighted_shift(curves[j + 1][2], curves[j][1], curves[j - 1][0], s0 - s1, s1 - s2)
    return shift + centred(y[j + 1], y[j], y[j - 1])


def curves_of(y, cells):
    return {m: curvature(y[m - 1], y[m], y[m + 1]) for m in cells}


def scales_of(cycles, first):
    edge = [(first + k).astype(f32) for k in range(cycles + 1)]
    scale = [(0.25 * time_step / 12.0) / (edge[k] + 0.5) for k in range(cycles)]
    return edge, scale


def outer_body(partial_ref, section_ref, pressure_ref, halo_ref, out_ref):
    cycles = section_ref.shape[1]
    row = lax.axis_index("row")
    last = row == lax.axis_size("row") - 1
    edge, scale = scales_of(cycles, row * cycles)
    for h in range(section_ref.shape[3] // LANES):
        lanes = slice(h * LANES, (h + 1) * LANES)

        def load(c, k):
            own = min(k, cycles - 1)
            mine = section_ref[c, own, :, lanes] if c < 6 else pressure_ref[own, :, lanes]
            if k < cycles:
                return mine
            return jnp.where(last, mine, halo_ref[c, k - cycles, :, lanes])

        for c, up, down in radial_parts(load, range(7)):
            cu = curves_of(up, (1, 2, 3, 4))
            cd = curves_of(down, (1, 2, 3, 4, 5))
            half_2 = edge[2] * face_down(down, 2, cd)
            face_3 = edge[3] * (face_up(up, 3, cu) + face_down(down, 3, cd))
            face_4 = edge[4] * (face_up(up, 4, cu) + face_down(down, 4, cd))
            out_ref[c, 0, :, lanes] = partial_ref[c, 0, :, lanes]
            out_ref[c, 1, :, lanes] = partial_ref[c, 1, :, lanes] - scale[1] * half_2
            out_ref[c, 2, :, lanes] = partial_ref[c, 2, :, lanes] - scale[2] * (face_3 - half_2)
            out_ref[c, 3, :, lanes] = partial_ref[c, 3, :, lanes] - scale[3] * (face_4 - face_3)


def inner_body(partial_ref, section_ref, pressure_ref, halo_ref, mirror_ref, out_ref):
    cycles = section_ref.shape[1]
    row = lax.axis_index("row")
    axis = row == 0
    edge, scale = scales_of(cycles, row * cycles)
    for h in range(section_ref.shape[3] // LANES):
        lanes = slice(h * LANES, (h + 1) * LANES)

        def load(c, k):
            if k >= 0:
                return section_ref[c, k, :, lanes] if c < 6 else pressure_ref[k, :, lanes]
            across = mirror_ref[c, -1 - k, :, lanes]
            if c in (1, 2):
                across = -across
            return jnp.where(axis, across, halo_ref[c, 3 + k, :, lanes])

        for c, up, down in radial_parts(load, range(-3, 4)):
            cu = curves_of(up, (-2, -1, 0, 1, 2))
            cd = curves_of(down, (-1, 0, 1, 2))
            face_0 = edge[0] * (face_up(up, 0, cu) + face_down(down, 0, cd))
            face_1 = edge[1] * (face_up(up, 1, cu) + face_down(down, 1, cd))
            half_2 = edge[2] * face_up(up, 2, cu)
            out_ref[c, 0, :, lanes] = partial_ref[c, 0, :, lanes] - scale[0] * (face_1 - face_0)
            out_ref[c, 1, :, lanes] = partial_ref[c, 1, :, lanes] - scale[1] * (half_2 - face_1)
            out_ref[c, 2, :, lanes] = partial_ref[c, 2, :, lanes] + scale[2] * half_2
            out_ref[c, 3, :, lanes] = partial_ref[c, 3, :, lanes]


def radial_call(body, partial, section, pressure, *halos):
    channels, cycles, depth, width = section.shape
    state = pl.BlockSpec((channels, cycles, SUB, width), lambda i: (0, 0, i, 0))
    halo = pl.BlockSpec((7, 3, SUB, width), lambda i: (0, 0, i, 0))
    return pl.pallas_call(
        body,
        out_shape=jax.ShapeDtypeStruct(partial.shape, f32),
        grid=(depth // SUB,),
        in_specs=[state, state, pl.BlockSpec((cycles, SUB, width), lambda i: (0, i, 0))]
        + [halo] * len(halos),
        out_specs=state,
    )(partial, section, pressure, *halos)


def build_table(positions, mode_count, length):
    orders = lax.iota(jnp.int32, mode_count)
    phases = positions[:, None] * orders[None, :] % length
    angles = phases.astype(jnp.float32) * (2.0 * math.pi / length)
    return jnp.concatenate([jnp.cos(angles), jnp.sin(angles)], 1)


def cycle_weights(cutoff, mode_count, length):
    orders = lax.iota(jnp.int32, mode_count)
    mode_scale = jnp.where(orders == 0, 1.0 / length, 2.0 / length)
    kept_modes = orders[None, :] <= cutoff[:, None]
    weight_half = jnp.where(kept_modes, mode_scale[None, :], 0.0)
    return jnp.concatenate([weight_half, weight_half], 1)


def sum_over_theta(coefficients, theta_id):
    half = coefficients.shape[2] // 2
    core = theta_id % 2
    core_swap = [(0, 1), (1, 0), (2, 3), (3, 2)]
    chip_swap = [(0, 2), (2, 0), (1, 3), (3, 1)]
    axes = ("row", "theta")
    low, high = coefficients[:, :, :half], coefficients[:, :, half:]
    mine = jnp.where(core == 0, low, high)
    other = jnp.where(core == 0, high, low)
    mine = mine + lax.ppermute(other, axes, core_swap)
    mine = mine + lax.ppermute(mine, axes, chip_swap)
    other = lax.ppermute(mine, axes, core_swap)
    low = jnp.where(core == 0, mine, other)
    high = jnp.where(core == 0, other, mine)
    return jnp.concatenate([low, high], 2)


def ring(count):
    up = [(i, (i + 1) % count) for i in range(count)]
    return up, [(b, a) for a, b in up]


def shards(state_start, state_section, phase, cutoff):
    row_count = lax.axis_size("row")
    row_id = lax.axis_index("row")
    theta_count = lax.axis_size("theta")
    theta_id = lax.axis_index("theta")
    gz_count = lax.axis_size("gz")

    bottom, top, pressure, z_first, z_last = pack_call(state_section, phase)
    across = [(t, (t + theta_count // 2) % theta_count) for t in range(theta_count)]
    mirror = lax.ppermute(bottom, ("row", "theta"), across)
    above = lax.ppermute(bottom, "row", [(r + 1, r) for r in range(row_count - 1)])
    turned, t_first, t_last = turn_call(state_section, pressure)
    up, down = ring(theta_count)
    t_before = lax.ppermute(t_last, "theta", up)
    t_after = lax.ppermute(t_first, "theta", down)
    below = lax.ppermute(top, "row", [(r, r + 1) for r in range(row_count - 1)])
    up, down = ring(gz_count)
    z_before = lax.ppermute(z_last, "gz", up)
    z_after = lax.ppermute(z_first, "gz", down)

    partial = axial_call(state_start, state_section, pressure, z_before, z_after)
    partial = swirl_call(partial, turned, t_before, t_after)
    partial = radial_call(outer_body, partial, state_section, pressure, above)
    advanced = radial_call(inner_body, partial, state_section, pressure, below, mirror)

    weights = cycle_weights(cutoff, KMODES, NT)
    local_theta = advanced.shape[3]
    positions = theta_id * local_theta + lax.iota(jnp.int32, local_theta)
    table = build_table(positions, KMODES, NT)
    exact = lax.Precision.HIGHEST
    coefficients = jnp.einsum("vizt,tk->vizk", advanced, table, precision=exact)
    coefficients = sum_over_theta(coefficients, theta_id)
    coefficients = coefficients * weights[None, :, None, :]
    filtered = jnp.einsum("vizk,tk->vizt", coefficients, table, precision=exact)
    return jnp.where(row_id == 0, filtered, advanced)


def solution(mesh):
    in_specs = (
        P(None, "row", "gz", "theta"),
        P(None, "row", "gz", "theta"),
        P("row", "gz", "theta"),
        P(),
    )
    out_specs = P(None, "row", "gz", "theta")
    return jax.shard_map(shards, mesh=mesh, in_specs=in_specs, out_specs=out_specs, check_vma=False)
```
